256 devices in a mesh: gx: 8 (over x, core), gy: 4 (over z_hi), gz: 8 (over z_lo, y).
Axes of the slice: x: 4, y: 4, z: 8 (z_hi: 4, z_lo: 2; z = z_hi * 2 + z_lo), core: 2. Of those that a mesh axis runs over, the one named last changes fastest.
Arguments:
- hidden_rows: bfloat16 [4096, 16384], P(('gx', 'gy'), 'gz'), may hold values from -2000 to 2000
- norm_gain: bfloat16 [16384], P('gz'), may hold values from 0.5 to 1.5
- w_query: bfloat16 [16384, 16384], P('gz', ('gx', 'gy')), may hold values from -0.046875 to 0.046875
- w_keyval: bfloat16 [16384, 2048], P('gz', ('gx', 'gy')), may hold values from -0.046875 to 0.046875
- positions: int32 [4096], P('gz'), may hold values from 0 to 1023, as said below
- keyval_order: int32 [8], replicated, may hold values from 0 to 7, each once
Outputs:
- queries: bfloat16 [4096, 16384], P('gz', ('gx', 'gy'))
- keyval_owned: bfloat16 [8, 4096, 256], P('gy', 'gz')
The draws below stay inside these ranges and needn't reach their ends.
Inputs may be any that keep to these rules, and one draw needn't show every extreme that they name: `positions`: each token's position within its packed document: 0 where a document starts, else one more than the previous token's; a document holds at most 1024 tokens. `keyval_order`: each head once.
All inputs are finite; a program needn't handle non-finite values.
Results may differ from the reference program's by a relative error of at most 0.0066.
Values may be sent and summed in bfloat16 or wider, within the bound.
No kernel may reach another device: no remote copies, remote signals or barrier semaphores. Data moves between devices by JAX's collectives and lax.ppermute only.
A program may use at most 128 MiB of HBM per device.

```python
import math
import jax
import jax.numpy as jnp
from jax import lax

D = 16384
HQ = 128
KVH = 8
HD = 128
TOKENS = 4096


def draw_hidden_rows(key, part):
    key_rows, key_cols, key_base = jax.random.split(key, 3)
    row_scale = jnp.exp(jax.random.uniform(key_rows, (TOKENS, 1), jnp.float32, 0.0, math.log(10.0)))
    col_place = jnp.arange(D, dtype=jnp.float32) / D
    col_scale = jnp.exp(math.log(3.0) * col_place + jax.random.uniform(key_cols, (D,), jnp.float32, 0.0, math.log(10.0)))
    base_values = jnp.clip(jax.random.normal(key_base, (TOKENS, D), jnp.float32), -6.0, 6.0)
    scaled_values = jnp.clip(base_values * row_scale * col_scale[None, :], -2000.0, 2000.0)
    return scaled_values.astype(jnp.bfloat16)


def draw_positions(key, part):
    longest = TOKENS // 4
    spacing = min(512, max(4, longest // 2))
    marks = jax.random.randint(key, (TOKENS,), 0, spacing)
    index_all = jnp.arange(TOKENS, dtype=jnp.int32)
    is_start = (marks == 0) & (index_all >= longest) | (index_all % longest == 0)
    starts = jnp.where(is_start, index_all, 0)
    return (index_all - lax.cummax(starts, axis=0)).astype(jnp.int32)


def level_of(stream_key, shape, pieces, least, largest):
    def one(dim, blocks):
        draws = jax.random.uniform(jax.random.fold_in(jax.random.fold_in(stream_key, 6), dim), (blocks,), jnp.float32, least / len(pieces), largest / len(pieces))
        return jnp.repeat(jnp.exp(draws), shape[dim] // blocks).reshape((-1,) + (1,) * (len(shape) - dim - 1))

    factor_of = one(*pieces[0])
    for cut in pieces[1:]:
        factor_of = factor_of * one(*cut)
    return factor_of


def normal_values(stream_key, dims, deviation, limit, cuts=(), kind=jnp.bfloat16):
    entries = deviation * jax.random.normal(stream_key, dims, jnp.float32)
    if cuts:
        entries = entries * level_of(stream_key, dims, cuts, -0.22, 0.18)
    return jnp.clip(entries, -limit, limit).astype(kind)


def setup_inputs(seed: int = 0) -> dict:
    key_of = jax.random.split(jax.random.key(seed), 7)
    hidden_rows = draw_hidden_rows(jax.random.fold_in(key_of[6], 71), 0)
    norm_gain = jnp.clip(1.0 + 0.1 * jax.random.normal(key_of[1], (D,), jnp.float32), 0.5, 1.5).astype(jnp.bfloat16)
    w_query = normal_values(key_of[2], (D, HQ * HD), D ** -0.5, 0.046875, ((0, 8), (1, 32)))
    w_keyval = normal_values(key_of[3], (D, 2 * KVH * HD), D ** -0.5, 0.046875, ((0, 8), (1, 32)))
    positions = draw_positions(jax.random.fold_in(key_of[6], 71), 0)
    keyval_order = jax.random.permutation(key_of[5], KVH).astype(jnp.int32)
    return {"hidden_rows": hidden_rows, "norm_gain": norm_gain, "w_query": w_query, "w_keyval": w_keyval, "positions": positions, "keyval_order": keyval_order}


rope_base = 500000.0
norm_eps = 1e-05

def rotate_heads(values, position_ids):
    pair_index = jnp.arange(HD // 2, dtype=jnp.float32)
    inv_freq = jnp.exp(pair_index * (-2.0 * math.log(rope_base) / HD))
    angles = position_ids.astype(jnp.float32)[:, None] * inv_freq[None, :]
    cosines = jnp.cos(angles)[:, None, :]
    sine_part = jnp.sin(angles)[:, None, :]
    paired = values.reshape(values.shape[0], values.shape[1], HD // 2, 2)
    even_part = paired[..., 0]
    odd_part = paired[..., 1]
    rotated = jnp.stack([even_part * cosines - odd_part * sine_part, even_part * sine_part + odd_part * cosines], axis=-1)
    return rotated.reshape(values.shape)

def reference(hidden_rows, norm_gain, w_query, w_keyval, positions, keyval_order):
    widened = hidden_rows.astype(jnp.float32)
    mean_square = lax.optimization_barrier(jnp.sum(widened * widened, axis=1)) / D
    normed = (widened * lax.rsqrt(mean_square + norm_eps)[:, None] * norm_gain.astype(jnp.float32)).astype(jnp.bfloat16)
    query_raw = jnp.dot(normed, w_query, preferred_element_type=jnp.float32)
    queries = rotate_heads(query_raw.reshape(TOKENS, HQ, HD), positions).reshape(TOKENS, HQ * HD).astype(jnp.bfloat16)
    keyval_raw = jnp.dot(normed, w_keyval, preferred_element_type=jnp.float32).reshape(TOKENS, KVH, 2, HD)
    key_rot = rotate_heads(keyval_raw[:, :, 0, :], positions)
    keyval_rot = jnp.stack([key_rot, keyval_raw[:, :, 1, :]], axis=2).reshape(TOKENS, KVH, 2 * HD).astype(jnp.bfloat16)
    keyval_owned = jnp.transpose(keyval_rot[:, keyval_order, :], (1, 0, 2))
    return (queries, keyval_owned)
```

```python
import functools
import math

import jax
import jax.numpy as jnp
from jax import lax
from jax.experimental import pallas as pl
from jax.experimental.pallas import tpu as pltpu
from jax.sharding import PartitionSpec as P

D = 16384
HD = 128
ROPE_BASE = 500000.0
NORM_EPS = 1e-05
AXES = ("gx", "gy", "gz")


BACK = (0, 2, 3, 1)
GROUPS = ((0,), (1,), (2, 3))

F32 = jnp.float32
BF16 = jnp.bfloat16


def moves(rule):
    pairs = []
    for x in range(4):
        for core in range(2):
            for zh in range(4):
                a, b, c = rule(x, core, zh)
                for k in range(8):
                    target = (((a % 4) * 2 + b) * 4 + c % 4) * 8 + k
                    pairs.append((((x * 2 + core) * 4 + zh) * 8 + k, target))
    return pairs


def send(value, rule):
    return lax.ppermute(value, AXES, moves(rule))


def along_z(step):
    return lambda x, c, zh: (x, c, zh + step)


def along_x(step):
    return lambda x, c, zh: (x + step, c, zh)


def other_core(x, c, zh):
    return (x, 1 - c, zh)


def exchange(value, axis):
    return lax.all_to_all(value, axis, 0, 0, tiled=True)


def gray(v):
    return v ^ (v >> 1)


def spread_kv(kv):
    kv = kv[None]
    steps = (
        lambda x, c, zh: (x, c, zh ^ 1),
        lambda x, c, zh: (x, c, zh ^ 3),
        lambda x, c, zh: (x ^ 1, c, zh),
        lambda x, c, zh: (x ^ 3, c, zh),
        other_core,
    )
    for rule in steps:
        kv = jnp.concatenate([kv, send(kv, rule)])
    return kv


def vmem(count):
    return [pl.BlockSpec(memory_space=pltpu.VMEM)] * count


def smem():
    return pl.BlockSpec(memory_space=pltpu.SMEM)


def prepare_kernel(wq, wk, gain, out):
    width = wq.shape[1]
    g = gain[...]
    for k in range(0, width, 128):
        out[:, k : k + 128] = (wq[:, k : k + 128].astype(F32) * g).astype(BF16)
    kv = (wk[...].astype(F32) * g).astype(BF16)
    out[:, width : width + 64] = kv
    out[:, width + 64 :] = kv


def prepare(wq, wk, gain):
    return pl.pallas_call(
        prepare_kernel,
        out_shape=jax.ShapeDtypeStruct((wq.shape[0], wq.shape[1] + 128), BF16),
        in_specs=vmem(3),
        out_specs=vmem(1)[0],
        cost_estimate=pl.CostEstimate(flops=1 << 20, bytes_accessed=5 << 20, transcendentals=0),
        name="prepare",
    )(wq, wk, gain)


def project_kernel(count, at, *refs):
    parts, (wa, wb, wk), outs = refs[: 4 * count], refs[4 * count : 4 * count + 3], refs[4 * count + 3 : -6]
    rows, a_held, b_held, k_held, row_sems, w_sems = refs[-6:]
    q_out, kv_out = outs[0], outs[-1]
    width = a_held.shape[1]
    base = 2 * width if len(outs) == 1 else 0
    a_copy = pltpu.make_async_copy(wa.at[:, :width], a_held, w_sems.at[0])
    b_copy = pltpu.make_async_copy(wb.at[:, :width], b_held, w_sems.at[1])
    k_copy = pltpu.make_async_copy(wk, k_held, w_sems.at[2])
    a_copy.start()
    row_copies = []
    for p in range(count):
        for i in range(4):
            for core in range(2):
                there = (at[i] * 2 + core) * 64 * count + p * 64
                there = rows.at[pl.ds(pl.multiple_of(there, 64), 64), :]
                here = parts[p * 4 + i].at[core * 64 : (core + 1) * 64, :]
                row_copies.append(pltpu.make_async_copy(here, there, row_sems.at[len(row_copies)]))
    for copy in row_copies:
        copy.start()
    a_copy.wait()
    for copy in row_copies:
        copy.wait()
    b_copy.start()
    k_copy.start()
    size = 256

    def first(i, carry):
        there = pl.ds(pl.multiple_of(i * size, size), size)
        q_out[there, :width] = jnp.dot(rows[there, :], a_held[...], preferred_element_type=F32).astype(BF16)
        for part in range(0, size, 128):
            there = pl.ds(pl.multiple_of(i * size + part, 128), 128)
            squares = jnp.zeros((128, 128), F32)
            for k in range(0, rows.shape[1], 128):
                v = rows[there, k : k + 128].astype(F32)
                squares = squares + v * v
            sums = jnp.broadcast_to(jnp.sum(squares, axis=1, keepdims=True), (128, 128))
            high = sums.astype(BF16).astype(F32)
            lane = lax.broadcasted_iota(jnp.int32, (128, 128), 1)
            kv_out[there, base + 128 : base + 256] = jnp.where(lane < 64, high, sums - high).astype(BF16)
        return carry

    def second(i, carry):
        there = pl.ds(pl.multiple_of(i * size, size), size)
        kv_out[there, base : base + 128] = jnp.dot(
            rows[there, :], k_held[...], preferred_element_type=F32
        ).astype(BF16)
        q_out[there, width : 2 * width] = jnp.dot(
            rows[there, :], b_held[...], preferred_element_type=F32
        ).astype(BF16)
        return carry

    lax.fori_loop(0, rows.shape[0] // size, first, 0)
    b_copy.wait()
    k_copy.wait()
    lax.fori_loop(0, rows.shape[0] // size, second, 0)


def project(at, parts, weights, split):
    depth, width = weights[0].shape[0], weights[0].shape[1] - 128
    widths = (2 * width, 256) if split else (2 * width + 256,)
    count = len(parts) // 4
    return pl.pallas_call(
        functools.partial(project_kernel, count),
        out_shape=tuple(jax.ShapeDtypeStruct((512 * count, v), BF16) for v in widths),
        in_specs=[smem()] + [pl.BlockSpec(memory_space=pl.ANY)] * (4 * count + 3),
        out_specs=tuple(vmem(len(widths))),
        scratch_shapes=[
            pltpu.VMEM((512 * count, depth), BF16),
            pltpu.VMEM((depth, width), BF16),
            pltpu.VMEM((depth, width), BF16),
            pltpu.VMEM((depth, 128), BF16),
            pltpu.SemaphoreType.DMA((8 * count,)),
            pltpu.SemaphoreType.DMA((3,)),
        ],
        cost_estimate=pl.CostEstimate(
            flops=2 * 512 * count * depth * 1152, bytes_accessed=(5 + 3 * count) << 20, transcendentals=0
        ),
    )(at, *parts, *weights)


def turn(v, cosines, sines):
    lane = lax.broadcasted_iota(jnp.int32, v.shape, 1)
    swapped = jnp.where(lane % 2 == 0, pltpu.roll(v, 127, 1), pltpu.roll(v, 1, 1))
    return v * cosines + swapped * sines


def total(ref, lo):
    got = ref[0, :, lo : lo + 128].astype(F32)
    for k in range(1, ref.shape[0]):
        got = got + ref[k, :, lo : lo + 128].astype(F32)
    return got


def factor_of(ref, lo):
    squares = total(ref, lo)
    return lax.rsqrt((squares[:, 0:1] + squares[:, 64:65]) / D + NORM_EPS)


def joined(refs):
    return jnp.concatenate([v[...] for v in refs], axis=0)


def write_q(came, factor, cos, sin, q_own, q_other):
    width = q_own.shape[1]
    cosines, sines = joined(cos) * factor, joined(sin) * factor
    for h in range(2 * width // 128):
        got = turn(total(came, h * 128), cosines, sines).astype(BF16)
        if h * 128 < width:
            q_own[:, h * 128 : (h + 1) * 128] = got
        else:
            q_other[:, h * 128 - width : (h + 1) * 128 - width] = got


def write_kv(came, lo, factor, cos, sin, kv):
    kv[...] = turn(total(came, lo), joined(cos) * factor, joined(sin) * factor).astype(BF16)


def finish_kernel(n, at, came, *refs):
    tables, (q_own, q_other, kv) = [refs[k * n : k * n + n] for k in range(4)], refs[4 * n :]
    base = 2 * q_own.shape[1]
    factor = factor_of(came, base + 128)
    write_q(came, factor, *tables[:2], q_own, q_other)
    write_kv(came, base, factor, *tables[2:], kv)


def finish_kv_kernel(n, at, came, *refs):
    write_kv(came, 0, factor_of(came, 128), refs[:n], refs[n : 2 * n], refs[2 * n])


def finish_q_kernel(n, at, came, came_kv, *refs):
    write_q(came, factor_of(came_kv, 128), refs[:n], refs[n : 2 * n], *refs[2 * n :])


def finish(kernel, rows, came, tables, widths, group):
    block = came[0].shape[1]

    def table(part):
        return pl.BlockSpec((64, 128), lambda n, at: (at[part], 0))

    parts = GROUPS[group]
    return pl.pallas_call(
        functools.partial(kernel, len(parts)),
        out_shape=tuple(jax.ShapeDtypeStruct((block, v), BF16) for v in widths),
        grid_spec=pltpu.PrefetchScalarGridSpec(
            num_scalar_prefetch=1,
            grid=(1,),
            in_specs=[pl.BlockSpec(v.shape, lambda n, at: (0, 0, 0)) for v in came]
            + [table(p) for _ in tables for p in parts],
            out_specs=tuple(pl.BlockSpec((block, v), lambda n, at: (0, 0)) for v in widths),
        ),
        cost_estimate=pl.CostEstimate(flops=1 << 20, bytes_accessed=2 << 20, transcendentals=0),
    )(rows, *came, *[v for v in tables for _ in parts])


def last_kernel(at, pick, q_near, q_far, q_near_came, q_far_came, kv, q_out, kv_out):
    lane = lax.broadcasted_iota(jnp.int32, (64, 128), 1)
    for p in range(4):
        here = slice(p % 2 * 64, p % 2 * 64 + 64)
        rows = pl.ds(pl.multiple_of(at[p] * 64, 64), 64)
        q_out[rows, :] = (q_near, q_far)[p // 2][here, :]
        rows = pl.ds(pl.multiple_of(at[4 + p] * 64, 64), 64)
        q_out[rows, :] = (q_near_came, q_far_came)[p // 2][here, :]
    for s in range(2):
        x_off, odd = pick[4 + 2 * s], pick[5 + 2 * s]
        for t in range(4):
            for core in range(2):

                def part(g, t=t, core=core, x_off=x_off):
                    i = BACK[(t - g) % 4]
                    return kv[pick[8 + core] + x_off + pick[g], i * 64 : (i + 1) * 64, :].astype(F32)

                for half in range(2):
                    a, b = part(2 * half), part(2 * half + 1)
                    low = jnp.where(odd == 0, a, pltpu.roll(a, 64, 1))
                    high = jnp.where(odd == 0, pltpu.roll(b, 64, 1), b)
                    kv_out[s, t * 128 + core * 64 : t * 128 + core * 64 + 64, half * 128 : (half + 1) * 128] = jnp.where(
                        lane < 64, low, high
                    ).astype(BF16)


def last(at, pick, arrays, tokens):
    return pl.pallas_call(
        last_kernel,
        out_shape=(
            jax.ShapeDtypeStruct((tokens, arrays[0].shape[1]), BF16),
            jax.ShapeDtypeStruct((2, tokens, 256), BF16),
        ),
        in_specs=[smem(), smem()] + vmem(len(arrays)),
        out_specs=tuple(vmem(2)),
        cost_estimate=pl.CostEstimate(flops=1 << 10, bytes_accessed=4 << 20, transcendentals=0),
        name="last",
    )(at, pick, *arrays)


def spread_x(v, way):
    left, right = send(v, along_x(1)), send(v, along_x(-1))
    return [v, left, right, send(left if way > 0 else right, along_x(way))]


def body(hidden_rows, norm_gain, w_query, w_keyval, positions, keyval_order):
    gx, gy = (lax.axis_index(a).astype(jnp.int32) for a in AXES[:2])
    x, core = gx // 2, gx % 2
    width = w_query.shape[1]
    tokens = positions.shape[0]

    away = lax.dynamic_slice_in_dim(hidden_rows, (1 - core) * 64, 64, 0)
    home = lax.dynamic_slice_in_dim(hidden_rows, core * 64, 64, 0)
    came = send(away, other_core)
    mine = jnp.where(core == 0, jnp.concatenate([home, came]), jnp.concatenate([came, home]))

    gain = norm_gain.astype(F32)[:, None]
    mine_w = prepare(w_query, w_keyval, gain)
    other_w = send(mine_w, other_core)
    lane = lax.broadcasted_iota(jnp.int32, (1, 128), 1)
    weights = (mine_w, other_w, jnp.where(lane // 64 == core, mine_w[:, width:], other_w[:, width:]))

    def tables(column, is_key):
        inv_freq = jnp.exp((column // 2).astype(F32) * (-2.0 * math.log(ROPE_BASE) / HD))
        angles = positions.astype(F32)[:, None] * inv_freq
        sign = jnp.where(column % 2 == 0, -1.0, 1.0)
        return jnp.where(is_key, jnp.cos(angles), 1.0), jnp.where(is_key, jnp.sin(angles) * sign, 0.0)

    all_tables = (*tables(lane, True), *tables((gy % 2) * 64 + lane % 64, gy < 2))

    ring = jnp.array([0, 3, 1, 2], jnp.int32)
    place = (x + ring) % 4
    source_z = (gy + ring) % 4
    at = jnp.concatenate([source_z * 2 + core, source_z * 2 + 1 - core])
    wanted = lax.dynamic_slice_in_dim(keyval_order, gy * 2, 2, 0)
    four, two = jnp.arange(4, dtype=jnp.int32), jnp.arange(2, dtype=jnp.int32)
    pick = jnp.concatenate(
        [gray(four ^ gy), jnp.stack([gray(wanted // 2 ^ x) * 4, wanted % 2], axis=1).reshape(4), (two ^ core) * 16]
    )

    left, right = send(mine, along_z(1)), send(mine, along_z(-1))
    far = send(left, along_z(1))
    chunks = [spread_x(v, 1 - 2 * (p % 2)) for p, v in enumerate((mine, left, right, far))]
    q_own, q_other, kvs = [], [], []
    for n, group in enumerate(GROUPS):
        split = n + 1 == len(GROUPS)
        sums = project(place, [v for p in group for v in chunks[p]], weights, split)
        sums = [v.reshape(8, v.shape[0] // 8, v.shape[1]) for v in sums]
        if split:
            few = exchange(sums[1], "gz")
            many = exchange(sums[0], "gz")
            (kv,) = finish(finish_kv_kernel, at, (few,), all_tables[2:], (128,), n)
            own, other = finish(finish_q_kernel, at, (many, few), all_tables[:2], (width, width), n)
        else:
            came = exchange(sums[0], "gz")
            own, other, kv = finish(finish_kernel, at, (came,), all_tables, (width, width, 128), n)
        q_own.append(own)
        q_other.append(other)
        kvs.append(kv)
    q_near = jnp.concatenate(q_own[:2])
    q_near_came = send(jnp.concatenate(q_other[:2]), other_core)
    q_far_came = send(q_other[2], other_core)
    kv = spread_kv(jnp.concatenate(kvs))
    return last(at, pick, (q_near, q_own[2], q_near_came, q_far_came, kv), tokens)


def solution(mesh):
    in_specs = (
        P(("gx", "gy"), "gz"),
        P("gz"),
        P("gz", ("gx", "gy")),
        P("gz", ("gx", "gy")),
        P("gz"),
        P(),
    )
    out_specs = (P("gz", ("gx", "gy")), P("gy", "gz", None))

    return jax.shard_map(body, mesh=mesh, in_specs=in_specs, out_specs=out_specs, check_vma=False)
```

```python
import functools
import math

import jax
import jax.numpy as jnp
from jax import lax
from jax.experimental import pallas as pl
from jax.experimental.pallas import tpu as pltpu
from jax.sharding import PartitionSpec as P

D = 16384
HD = 128
ROPE_BASE = 500000.0
NORM_EPS = 1e-05
AXES = ("gx", "gy", "gz")


BACK = (0, 2, 3, 1)
GROUPS = ((0,), (1,), (2, 3))

F32 = jnp.float32
BF16 = jnp.bfloat16


def moves(rule):
    pairs = []
    for x in range(4):
        for core in range(2):
            for zh in range(4):
                a, b, c = rule(x, core, zh)
                for k in range(8):
                    target = (((a % 4) * 2 + b) * 4 + c % 4) * 8 + k
                    pairs.append((((x * 2 + core) * 4 + zh) * 8 + k, target))
    return pairs


def send(value, rule):
    return lax.ppermute(value, AXES, moves(rule))


def along_z(step):
    return lambda x, c, zh: (x, c, zh + step)


def along_x(step):
    return lambda x, c, zh: (x + step, c, zh)


def other_core(x, c, zh):
    return (x, 1 - c, zh)


def exchange(value, axis):
    return lax.all_to_all(value, axis, 0, 0, tiled=True)


def gray(v):
    return v ^ (v >> 1)


def spread_kv(kv):
    kv = kv[None]
    for step in (1, 3):
        kv = jnp.concatenate([kv, send(kv, lambda x, c, zh, step=step: (x, c, zh ^ step))])
    near = send(kv, lambda x, c, zh: (x ^ 1, c, zh))
    back = send(kv, lambda x, c, zh: (x ^ 3, c, zh))
    return kv, near, back, send(near, lambda x, c, zh: (x ^ 3, c, zh))


def vmem(count):
    return [pl.BlockSpec(memory_space=pltpu.VMEM)] * count


def smem():
    return pl.BlockSpec(memory_space=pltpu.SMEM)


def prepare_kernel(wq, wk, gain, out):
    width = wq.shape[1]
    g = gain[...]
    for k in range(0, width, 128):
        out[:, k : k + 128] = (wq[:, k : k + 128].astype(F32) * g).astype(BF16)
    kv = (wk[...].astype(F32) * g).astype(BF16)
    out[:, width : width + 64] = kv
    out[:, width + 64 :] = kv


def prepare(wq, wk, gain):
    return pl.pallas_call(
        prepare_kernel,
        out_shape=jax.ShapeDtypeStruct((wq.shape[0], wq.shape[1] + 128), BF16),
        in_specs=vmem(3),
        out_specs=vmem(1)[0],
        cost_estimate=pl.CostEstimate(flops=1 << 20, bytes_accessed=5 << 20, transcendentals=0),
        name="prepare",
    )(wq, wk, gain)


def small(size):
    return pltpu.CompilerParams(vmem_limit_bytes=size << 20)


def project_kernel(count, at, *refs):
    parts, (wa, wb), outs = refs[: 4 * count], refs[4 * count : 4 * count + 2], refs[4 * count + 2 : -7]
    rows, a_held, b_held, ka_held, kb_held, row_sems, w_sems = refs[-7:]
    q_out, kv_out = outs[0], outs[-1]
    width = a_held.shape[1]
    base = 2 * width if len(outs) == 1 else 0
    a_copy = pltpu.make_async_copy(wa.at[:, :width], a_held, w_sems.at[0])
    later = [
        pltpu.make_async_copy(wb.at[:, :width], b_held, w_sems.at[1]),
        pltpu.make_async_copy(wa.at[:, width:], ka_held, w_sems.at[2]),
        pltpu.make_async_copy(wb.at[:, width:], kb_held, w_sems.at[3]),
    ]
    row_copies = []
    for p in range(count):
        for i in range(4):
            there = rows.at[p, pl.ds(pl.multiple_of(at[i] * 128, 128), 128), :]
            row_copies.append(pltpu.make_async_copy(parts[p * 4 + i], there, row_sems.at[len(row_copies)]))
    a_copy.start()
    for copy in row_copies[:4]:
        copy.start()
    a_copy.wait()
    for copy in row_copies[:4]:
        copy.wait()
    for copy in row_copies[4:] + later:
        copy.start()
    size = 256

    def store(out, p, i, lanes, got):
        for k in range(size // 64):
            there = pl.ds(pl.multiple_of((i * (size // 64) + k) * 64 * count + p * 64, 64), 64)
            out[there, lanes] = got[k * 64 : (k + 1) * 64]

    def first(p, i, carry):
        here = pl.ds(pl.multiple_of(i * size, size), size)
        got = jnp.dot(rows[p, here, :], a_held[...], preferred_element_type=F32).astype(BF16)
        store(q_out, p, i, slice(0, width), got)
        squares = jnp.zeros((size, 128), F32)
        for k in range(0, rows.shape[2], 128):
            v = rows[p, here, k : k + 128].astype(F32)
            squares = squares + v * v
        sums = jnp.broadcast_to(jnp.sum(squares, axis=1, keepdims=True), (size, 128))
        high = sums.astype(BF16).astype(F32)
        lane = lax.broadcasted_iota(jnp.int32, (size, 128), 1)
        store(kv_out, p, i, slice(base + 128, base + 256), jnp.where(lane < 64, high, sums - high).astype(BF16))
        return carry

    def second(p, i, carry):
        here = pl.ds(pl.multiple_of(i * size, size), size)
        got = jnp.dot(rows[p, here, :], b_held[...], preferred_element_type=F32).astype(BF16)
        store(q_out, p, i, slice(width, 2 * width), got)
        got = jnp.dot(rows[p, here, :], ka_held[...], preferred_element_type=F32).astype(BF16)
        store(kv_out, p, i, slice(base, base + 128), got)
        return carry

    for p in range(count):
        if p:
            for copy in row_copies[4 * p : 4 * p + 4]:
                copy.wait()
        lax.fori_loop(0, 512 // size, functools.partial(first, p), 0)
    for copy in later:
        copy.wait()
    lane = lax.broadcasted_iota(jnp.int32, ka_held.shape, 1)
    ka_held[...] = jnp.where(lane // 64 == at[4], ka_held[...].astype(F32), kb_held[...].astype(F32)).astype(BF16)
    for p in range(count):
        lax.fori_loop(0, 512 // size, functools.partial(second, p), 0)


def project(at, parts, weights, split):
    depth, width = weights[0].shape[0], weights[0].shape[1] - 128
    widths = (2 * width, 256) if split else (2 * width + 256,)
    count = len(parts) // 4
    return pl.pallas_call(
        functools.partial(project_kernel, count),
        out_shape=tuple(jax.ShapeDtypeStruct((512 * count, v), BF16) for v in widths),
        in_specs=[smem()] + [pl.BlockSpec(memory_space=pl.ANY)] * (4 * count + 2),
        out_specs=tuple(vmem(len(widths))),
        scratch_shapes=[
            pltpu.VMEM((count, 512, depth), BF16),
            pltpu.VMEM((depth, width), BF16),
            pltpu.VMEM((depth, width), BF16),
            pltpu.VMEM((depth, 128), BF16),
            pltpu.VMEM((depth, 128), BF16),
            pltpu.SemaphoreType.DMA((4 * count,)),
            pltpu.SemaphoreType.DMA((4,)),
        ],
        cost_estimate=pl.CostEstimate(
            flops=2 * 512 * count * depth * 1152, bytes_accessed=(5 + 3 * count) << 20, transcendentals=0
        ),
    )(at, *parts, *weights)


def turn(v, cosines, sines):
    lane = lax.broadcasted_iota(jnp.int32, v.shape, 1)
    swapped = jnp.where(lane % 2 == 0, pltpu.roll(v, 127, 1), pltpu.roll(v, 1, 1))
    return v * cosines + swapped * sines


def total(ref, lo):
    got = ref[0, :, lo : lo + 128].astype(F32)
    for k in range(1, ref.shape[0]):
        got = got + ref[k, :, lo : lo + 128].astype(F32)
    return got


def factor_of(ref, lo):
    squares = total(ref, lo)
    return lax.rsqrt((squares[:, 0:1] + squares[:, 64:65]) / D + NORM_EPS)


def joined(refs):
    return jnp.concatenate([v[...] for v in refs], axis=0)


def write_q(came, factor, cos, sin, q_own, q_other):
    width = q_own.shape[1]
    cosines, sines = joined(cos) * factor, joined(sin) * factor
    for h in range(2 * width // 128):
        got = turn(total(came, h * 128), cosines, sines).astype(BF16)
        if h * 128 < width:
            q_own[:, h * 128 : (h + 1) * 128] = got
        else:
            q_other[:, h * 128 - width : (h + 1) * 128 - width] = got


def write_kv(came, lo, factor, cos, sin, kv):
    kv[...] = turn(total(came, lo), joined(cos) * factor, joined(sin) * factor).astype(BF16)


def finish_kernel(n, at, came, *refs):
    tables, (q_own, q_other, kv) = [refs[k * n : k * n + n] for k in range(4)], refs[4 * n :]
    base = 2 * q_own.shape[1]
    factor = factor_of(came, base + 128)
    write_q(came, factor, *tables[:2], q_own, q_other)
    write_kv(came, base, factor, *tables[2:], kv)


def finish_kv_kernel(n, at, came, *refs):
    write_kv(came, 0, factor_of(came, 128), refs[:n], refs[n : 2 * n], refs[2 * n])


def finish_q_kernel(n, at, came, came_kv, *refs):
    write_q(came, factor_of(came_kv, 128), refs[:n], refs[n : 2 * n], *refs[2 * n :])


def finish(kernel, rows, came, tables, widths, group):
    block = came[0].shape[1]

    def table(part):
        return pl.BlockSpec((64, 128), lambda n, at: (at[part], 0))

    parts = GROUPS[group]
    return pl.pallas_call(
        functools.partial(kernel, len(parts)),
        out_shape=tuple(jax.ShapeDtypeStruct((block, v), BF16) for v in widths),
        grid_spec=pltpu.PrefetchScalarGridSpec(
            num_scalar_prefetch=1,
            grid=(1,),
            in_specs=[pl.BlockSpec(v.shape, lambda n, at: (0, 0, 0)) for v in came]
            + [table(p) for _ in tables for p in parts],
            out_specs=tuple(pl.BlockSpec((block, v), lambda n, at: (0, 0)) for v in widths),
        ),
        cost_estimate=pl.CostEstimate(flops=1 << 20, bytes_accessed=2 << 20, transcendentals=0),
        compiler_params=small(24),
    )(rows, *came, *[v for v in tables for _ in parts])


def owned_kernel(pick, own, near, back, far, out):
    lane = lax.broadcasted_iota(jnp.int32, (64, 128), 1)
    for s in range(2):
        x_off, odd = pick[4 + 2 * s], pick[5 + 2 * s]

        def part(g, t, x_off=x_off):
            rows = slice(BACK[(t - g) % 4] * 64, BACK[(t - g) % 4] * 64 + 64)
            got = [v[pick[g], rows, :].astype(F32) for v in (own, near, far, back)]
            low = jnp.where(x_off == 0, got[0], got[1])
            return jnp.where(x_off < 2, low, jnp.where(x_off == 2, got[2], got[3]))

        for t in range(4):
            for half in range(2):
                a, b = part(2 * half, t), part(2 * half + 1, t)
                low = jnp.where(odd == 0, a, pltpu.roll(a, 64, 1))
                high = jnp.where(odd == 0, pltpu.roll(b, 64, 1), b)
                out[s, t * 64 : (t + 1) * 64, half * 128 : (half + 1) * 128] = jnp.where(lane < 64, low, high).astype(BF16)


def owned(pick, arrays):
    return pl.pallas_call(
        owned_kernel,
        out_shape=jax.ShapeDtypeStruct((2, 256, 256), BF16),
        in_specs=[smem()] + vmem(4),
        out_specs=vmem(1)[0],
        cost_estimate=pl.CostEstimate(flops=1 << 20, bytes_accessed=1 << 20, transcendentals=0),
        compiler_params=small(24),
        name="owned",
    )(pick, *arrays)


def last_kernel(at, pick, q_near, q_far, q_near_came, q_far_came, kv, kv_came, q_out, kv_out):
    for p in range(4):
        here = slice(p % 2 * 64, p % 2 * 64 + 64)
        rows = pl.ds(pl.multiple_of(at[p] * 64, 64), 64)
        q_out[rows, :] = (q_near, q_far)[p // 2][here, :]
        rows = pl.ds(pl.multiple_of(at[4 + p] * 64, 64), 64)
        q_out[rows, :] = (q_near_came, q_far_came)[p // 2][here, :]
    core = pick[8]
    for s in range(2):
        for t in range(4):
            here = slice(t * 64, (t + 1) * 64)
            kv_out[s, pl.ds(pl.multiple_of(t * 128 + core * 64, 64), 64), :] = kv[s, here, :]
            kv_out[s, pl.ds(pl.multiple_of(t * 128 + (1 - core) * 64, 64), 64), :] = kv_came[s, here, :]


def last(at, pick, arrays, tokens):
    return pl.pallas_call(
        last_kernel,
        out_shape=(
            jax.ShapeDtypeStruct((tokens, arrays[0].shape[1]), BF16),
            jax.ShapeDtypeStruct((2, tokens, 256), BF16),
        ),
        in_specs=[smem(), smem()] + vmem(len(arrays)),
        out_specs=tuple(vmem(2)),
        cost_estimate=pl.CostEstimate(flops=1 << 10, bytes_accessed=4 << 20, transcendentals=0),
        compiler_params=small(24),
        name="last",
    )(at, pick, *arrays)


def spread_x(v, way):
    left, right = send(v, along_x(1)), send(v, along_x(-1))
    return [v, left, right, send(left if way > 0 else right, along_x(way))]


def body(hidden_rows, norm_gain, w_query, w_keyval, positions, keyval_order):
    gx, gy = (lax.axis_index(a).astype(jnp.int32) for a in AXES[:2])
    x, core = gx // 2, gx % 2
    width = w_query.shape[1]
    tokens = positions.shape[0]

    away = lax.dynamic_slice_in_dim(hidden_rows, (1 - core) * 64, 64, 0)
    home = lax.dynamic_slice_in_dim(hidden_rows, core * 64, 64, 0)
    came = send(away, other_core)
    mine = jnp.where(core == 0, jnp.concatenate([home, came]), jnp.concatenate([came, home]))

    gain = norm_gain.astype(F32)[:, None]
    mine_w = prepare(w_query, w_keyval, gain)
    other_w = send(mine_w, other_core)
    lane = lax.broadcasted_iota(jnp.int32, (1, 128), 1)
    weights = (mine_w, other_w)

    def tables(column, is_key):
        inv_freq = jnp.exp((column // 2).astype(F32) * (-2.0 * math.log(ROPE_BASE) / HD))
        angles = positions.astype(F32)[:, None] * inv_freq
        sign = jnp.where(column % 2 == 0, -1.0, 1.0)
        return jnp.where(is_key, jnp.cos(angles), 1.0), jnp.where(is_key, jnp.sin(angles) * sign, 0.0)

    all_tables = (*tables(lane, True), *tables((gy % 2) * 64 + lane % 64, gy < 2))

    ring = jnp.array([0, 3, 1, 2], jnp.int32)
    place = jnp.concatenate([(x + ring) % 4, core[None]])
    source_z = (gy + ring) % 4
    at = jnp.concatenate([source_z * 2 + core, source_z * 2 + 1 - core])
    wanted = lax.dynamic_slice_in_dim(keyval_order, gy * 2, 2, 0)
    four = jnp.arange(4, dtype=jnp.int32)
    pick = jnp.concatenate(
        [gray(four ^ gy), jnp.stack([wanted // 2 ^ x, wanted % 2], axis=1).reshape(4), core[None]]
    )

    left, right = send(mine, along_z(1)), send(mine, along_z(-1))
    far = send(left, along_z(1))
    chunks = [spread_x(v, 1 - 2 * (p % 2)) for p, v in enumerate((mine, left, right, far))]
    q_own, q_other, kvs = [], [], []
    for n, group in enumerate(GROUPS):
        split = n + 1 == len(GROUPS)
        sums = project(place, [v for p in group for v in chunks[p]], weights, split)
        sums = [v.reshape(8, v.shape[0] // 8, v.shape[1]) for v in sums]
        if split:
            few = exchange(sums[1], "gz")
            many = exchange(sums[0], "gz")
            (kv,) = finish(finish_kv_kernel, at, (few,), all_tables[2:], (128,), n)
            own, other = finish(finish_q_kernel, at, (many, few), all_tables[:2], (width, width), n)
        else:
            came = exchange(sums[0], "gz")
            own, other, kv = finish(finish_kernel, at, (came,), all_tables, (width, width, 128), n)
        q_own.append(own)
        q_other.append(other)
        kvs.append(kv)
    q_near = jnp.concatenate(q_own[:2])
    q_near_came = send(jnp.concatenate(q_other[:2]), other_core)
    q_far_came = send(q_other[2], other_core)
    kv_parts = spread_kv(jnp.concatenate(kvs))
    kv = owned(pick, kv_parts)
    kv_came = send(kv, other_core)
    return last(at, pick, (q_near, q_own[2], q_near_came, q_far_came, kv, kv_came), tokens)


def solution(mesh):
    in_specs = (
        P(("gx", "gy"), "gz"),
        P("gz"),
        P("gz", ("gx", "gy")),
        P("gz", ("gx", "gy")),
        P("gz"),
        P(),
    )
    out_specs = (P("gz", ("gx", "gy")), P("gy", "gz", None))

    return jax.shard_map(body, mesh=mesh, in_specs=in_specs, out_specs=out_specs, check_vma=False)
```

```python
import functools
import math

import jax
import jax.numpy as jnp
from jax import lax
from jax.experimental import pallas as pl
from jax.experimental.pallas import tpu as pltpu
from jax.sharding import PartitionSpec as P

D = 16384
HD = 128
ROPE_BASE = 500000.0
NORM_EPS = 1e-05
AXES = ("gx", "gy", "gz")


BACK = (0, 2, 3, 1)
GROUPS = ((0,), (1,), (2, 3))

F32 = jnp.float32
BF16 = jnp.bfloat16


def moves(rule):
    pairs = []
    for x in range(4):
        for core in range(2):
            for zh in range(4):
                a, b, c = rule(x, core, zh)
                for k in range(8):
                    target = (((a % 4) * 2 + b) * 4 + c % 4) * 8 + k
                    pairs.append((((x * 2 + core) * 4 + zh) * 8 + k, target))
    return pairs


def send(value, rule):
    return lax.ppermute(value, AXES, moves(rule))


def along_z(step):
    return lambda x, c, zh: (x, c, zh + step)


def along_x(step):
    return lambda x, c, zh: (x + step, c, zh)


def other_core(x, c, zh):
    return (x, 1 - c, zh)


def exchange(value, axis):
    return lax.all_to_all(value, axis, 0, 0, tiled=True)


def spread_kv(kv, pick):
    along = [send(kv, along_z(step)) for step in (1, -1, 2)]
    slots = list(owned(pick, jnp.stack([kv, *along])))
    for name in ("kx0", "kx1"):
        for s in range(2):
            step = 1 if (name == "kx0") == (s == 0) else 3
            slots[s] = slots[s] + send(slots[s], lambda x, c, zh, step=step: (x ^ step, c, zh))
    return jnp.stack(slots)


def vmem(count):
    return [pl.BlockSpec(memory_space=pltpu.VMEM)] * count


def smem():
    return pl.BlockSpec(memory_space=pltpu.SMEM)


def prepare_kernel(wq, wk, gain, out):
    width = wq.shape[1]
    g = gain[...]
    for k in range(0, width, 128):
        out[:, k : k + 128] = (wq[:, k : k + 128].astype(F32) * g).astype(BF16)
    kv = (wk[...].astype(F32) * g).astype(BF16)
    out[:, width : width + 64] = kv
    out[:, width + 64 :] = kv


def prepare(wq, wk, gain):
    return pl.pallas_call(
        prepare_kernel,
        out_shape=jax.ShapeDtypeStruct((wq.shape[0], wq.shape[1] + 128), BF16),
        in_specs=vmem(3),
        out_specs=vmem(1)[0],
        cost_estimate=pl.CostEstimate(flops=1 << 20, bytes_accessed=5 << 20, transcendentals=0),
        name="prepare",
    )(wq, wk, gain)


def small(size):
    return pltpu.CompilerParams(vmem_limit_bytes=size << 20)


def project_kernel(count, at, *refs):
    parts, (wa, wb), outs = refs[: 4 * count], refs[4 * count : 4 * count + 2], refs[4 * count + 2 : -7]
    rows, a_held, b_held, ka_held, kb_held, row_sems, w_sems = refs[-7:]
    q_out, kv_out = outs[0], outs[-1]
    width = a_held.shape[1]
    base = 2 * width if len(outs) == 1 else 0
    a_copy = pltpu.make_async_copy(wa.at[:, :width], a_held, w_sems.at[0])
    later = [
        pltpu.make_async_copy(wb.at[:, :width], b_held, w_sems.at[1]),
        pltpu.make_async_copy(wa.at[:, width:], ka_held, w_sems.at[2]),
        pltpu.make_async_copy(wb.at[:, width:], kb_held, w_sems.at[3]),
    ]
    row_copies = []
    for p in range(count):
        for i in range(4):
            there = rows.at[p, pl.ds(pl.multiple_of(at[i] * 128, 128), 128), :]
            row_copies.append(pltpu.make_async_copy(parts[p * 4 + i], there, row_sems.at[len(row_copies)]))
    a_copy.start()
    for copy in row_copies[:4]:
        copy.start()
    a_copy.wait()
    for copy in row_copies[:4]:
        copy.wait()
    for copy in row_copies[4:] + later:
        copy.start()
    size = 256

    def store(out, p, i, lanes, got):
        for k in range(size // 64):
            there = pl.ds(pl.multiple_of((i * (size // 64) + k) * 64 * count + p * 64, 64), 64)
            out[there, lanes] = got[k * 64 : (k + 1) * 64]

    def first(p, i, carry):
        here = pl.ds(pl.multiple_of(i * size, size), size)
        got = jnp.dot(rows[p, here, :], a_held[...], preferred_element_type=F32).astype(BF16)
        store(q_out, p, i, slice(0, width), got)
        squares = jnp.zeros((size, 128), F32)
        for k in range(0, rows.shape[2], 128):
            v = rows[p, here, k : k + 128].astype(F32)
            squares = squares + v * v
        sums = jnp.broadcast_to(jnp.sum(squares, axis=1, keepdims=True), (size, 128))
        high = sums.astype(BF16).astype(F32)
        lane = lax.broadcasted_iota(jnp.int32, (size, 128), 1)
        store(kv_out, p, i, slice(base + 128, base + 256), jnp.where(lane < 64, high, sums - high).astype(BF16))
        return carry

    def second(p, i, carry):
        here = pl.ds(pl.multiple_of(i * size, size), size)
        got = jnp.dot(rows[p, here, :], b_held[...], preferred_element_type=F32).astype(BF16)
        store(q_out, p, i, slice(width, 2 * width), got)
        got = jnp.dot(rows[p, here, :], ka_held[...], preferred_element_type=F32).astype(BF16)
        store(kv_out, p, i, slice(base, base + 128), got)
        return carry

    for p in range(count):
        if p:
            for copy in row_copies[4 * p : 4 * p + 4]:
                copy.wait()
        lax.fori_loop(0, 512 // size, functools.partial(first, p), 0)
    for copy in later:
        copy.wait()
    lane = lax.broadcasted_iota(jnp.int32, ka_held.shape, 1)
    ka_held[...] = jnp.where(lane // 64 == at[4], ka_held[...].astype(F32), kb_held[...].astype(F32)).astype(BF16)
    for p in range(count):
        lax.fori_loop(0, 512 // size, functools.partial(second, p), 0)


def project(at, parts, weights, split):
    depth, width = weights[0].shape[0], weights[0].shape[1] - 128
    widths = (2 * width, 256) if split else (2 * width + 256,)
    count = len(parts) // 4
    return pl.pallas_call(
        functools.partial(project_kernel, count),
        out_shape=tuple(jax.ShapeDtypeStruct((512 * count, v), BF16) for v in widths),
        in_specs=[smem()] + [pl.BlockSpec(memory_space=pl.ANY)] * (4 * count + 2),
        out_specs=tuple(vmem(len(widths))),
        scratch_shapes=[
            pltpu.VMEM((count, 512, depth), BF16),
            pltpu.VMEM((depth, width), BF16),
            pltpu.VMEM((depth, width), BF16),
            pltpu.VMEM((depth, 128), BF16),
            pltpu.VMEM((depth, 128), BF16),
            pltpu.SemaphoreType.DMA((4 * count,)),
            pltpu.SemaphoreType.DMA((4,)),
        ],
        cost_estimate=pl.CostEstimate(
            flops=2 * 512 * count * depth * 1152, bytes_accessed=(5 + 3 * count) << 20, transcendentals=0
        ),
    )(at, *parts, *weights)


def turn(v, cosines, sines):
    lane = lax.broadcasted_iota(jnp.int32, v.shape, 1)
    swapped = jnp.where(lane % 2 == 0, pltpu.roll(v, 127, 1), pltpu.roll(v, 1, 1))
    return v * cosines + swapped * sines


def total(ref, lo):
    got = ref[0, :, lo : lo + 128].astype(F32)
    for k in range(1, ref.shape[0]):
        got = got + ref[k, :, lo : lo + 128].astype(F32)
    return got


def factor_of(ref, lo):
    squares = total(ref, lo)
    return lax.rsqrt((squares[:, 0:1] + squares[:, 64:65]) / D + NORM_EPS)


def joined(refs):
    return jnp.concatenate([v[...] for v in refs], axis=0)


def write_q(came, factor, cos, sin, q_own, q_other):
    width = q_own.shape[1]
    cosines, sines = joined(cos) * factor, joined(sin) * factor
    for h in range(2 * width // 128):
        got = turn(total(came, h * 128), cosines, sines).astype(BF16)
        if h * 128 < width:
            q_own[:, h * 128 : (h + 1) * 128] = got
        else:
            q_other[:, h * 128 - width : (h + 1) * 128 - width] = got


def write_kv(came, lo, factor, cos, sin, kv):
    kv[...] = turn(total(came, lo), joined(cos) * factor, joined(sin) * factor).astype(BF16)


def finish_kernel(n, at, came, *refs):
    tables, (q_own, q_other, kv) = [refs[k * n : k * n + n] for k in range(4)], refs[4 * n :]
    base = 2 * q_own.shape[1]
    factor = factor_of(came, base + 128)
    write_q(came, factor, *tables[:2], q_own, q_other)
    write_kv(came, base, factor, *tables[2:], kv)


def finish_kv_kernel(n, at, came, *refs):
    write_kv(came, 0, factor_of(came, 128), refs[:n], refs[n : 2 * n], refs[2 * n])


def finish_q_kernel(n, at, came, came_kv, *refs):
    write_q(came, factor_of(came_kv, 128), refs[:n], refs[n : 2 * n], *refs[2 * n :])


def finish(kernel, rows, came, tables, widths, group):
    block = came[0].shape[1]

    def table(part):
        return pl.BlockSpec((64, 128), lambda n, at: (at[part], 0))

    parts = GROUPS[group]
    return pl.pallas_call(
        functools.partial(kernel, len(parts)),
        out_shape=tuple(jax.ShapeDtypeStruct((block, v), BF16) for v in widths),
        grid_spec=pltpu.PrefetchScalarGridSpec(
            num_scalar_prefetch=1,
            grid=(1,),
            in_specs=[pl.BlockSpec(v.shape, lambda n, at: (0, 0, 0)) for v in came]
            + [table(p) for _ in tables for p in parts],
            out_specs=tuple(pl.BlockSpec((block, v), lambda n, at: (0, 0)) for v in widths),
        ),
        cost_estimate=pl.CostEstimate(flops=1 << 20, bytes_accessed=2 << 20, transcendentals=0),
        compiler_params=small(24),
    )(rows, *came, *[v for v in tables for _ in parts])


def owned_kernel(pick, kv, *outs):
    lane = lax.broadcasted_iota(jnp.int32, (64, 128), 1)
    for s in range(2):
        here, odd = pick[4 + 2 * s] == 0, pick[5 + 2 * s]

        def part(g, t):
            rows = slice(BACK[(t - g) % 4] * 64, BACK[(t - g) % 4] * 64 + 64)
            return kv[pick[g], rows, :].astype(F32)

        for t in range(4):
            for half in range(2):
                a, b = part(2 * half, t), part(2 * half + 1, t)
                low = jnp.where(odd == 0, a, pltpu.roll(a, 64, 1))
                high = jnp.where(odd == 0, pltpu.roll(b, 64, 1), b)
                got = jnp.where(here, jnp.where(lane < 64, low, high), 0.0)
                outs[s][t * 64 : (t + 1) * 64, half * 128 : (half + 1) * 128] = got.astype(BF16)


def owned(pick, kv):
    return pl.pallas_call(
        owned_kernel,
        out_shape=(jax.ShapeDtypeStruct((256, 256), BF16),) * 2,
        in_specs=[smem()] + vmem(1),
        out_specs=tuple(vmem(2)),
        cost_estimate=pl.CostEstimate(flops=1 << 20, bytes_accessed=1 << 20, transcendentals=0),
        compiler_params=small(24),
        name="owned",
    )(pick, kv)


def last_kernel(at, pick, q_near, q_far, q_near_came, q_far_came, kv, kv_came, q_out, kv_out):
    for p in range(4):
        here = slice(p % 2 * 64, p % 2 * 64 + 64)
        rows = pl.ds(pl.multiple_of(at[p] * 64, 64), 64)
        q_out[rows, :] = (q_near, q_far)[p // 2][here, :]
        rows = pl.ds(pl.multiple_of(at[4 + p] * 64, 64), 64)
        q_out[rows, :] = (q_near_came, q_far_came)[p // 2][here, :]
    core = pick[8]
    for s in range(2):
        for t in range(4):
            here = slice(t * 64, (t + 1) * 64)
            kv_out[s, pl.ds(pl.multiple_of(t * 128 + core * 64, 64), 64), :] = kv[s, here, :]
            kv_out[s, pl.ds(pl.multiple_of(t * 128 + (1 - core) * 64, 64), 64), :] = kv_came[s, here, :]


def last(at, pick, arrays, tokens):
    return pl.pallas_call(
        last_kernel,
        out_shape=(
            jax.ShapeDtypeStruct((tokens, arrays[0].shape[1]), BF16),
            jax.ShapeDtypeStruct((2, tokens, 256), BF16),
        ),
        in_specs=[smem(), smem()] + vmem(len(arrays)),
        out_specs=tuple(vmem(2)),
        cost_estimate=pl.CostEstimate(flops=1 << 10, bytes_accessed=4 << 20, transcendentals=0),
        compiler_params=small(24),
        name="last",
    )(at, pick, *arrays)


def spread_x(v, way):
    left, right = send(v, along_x(1)), send(v, along_x(-1))
    return [v, left, right, send(left if way > 0 else right, along_x(way))]


def body(hidden_rows, norm_gain, w_query, w_keyval, positions, keyval_order):
    gx, gy = (lax.axis_index(a).astype(jnp.int32) for a in AXES[:2])
    x, core = gx // 2, gx % 2
    width = w_query.shape[1]
    tokens = positions.shape[0]

    away = lax.dynamic_slice_in_dim(hidden_rows, (1 - core) * 64, 64, 0)
    home = lax.dynamic_slice_in_dim(hidden_rows, core * 64, 64, 0)
    came = send(away, other_core)
    mine = jnp.where(core == 0, jnp.concatenate([home, came]), jnp.concatenate([came, home]))

    gain = norm_gain.astype(F32)[:, None]
    mine_w = prepare(w_query, w_keyval, gain)
    other_w = send(mine_w, other_core)
    lane = lax.broadcasted_iota(jnp.int32, (1, 128), 1)
    weights = (mine_w, other_w)

    def tables(column, is_key):
        inv_freq = jnp.exp((column // 2).astype(F32) * (-2.0 * math.log(ROPE_BASE) / HD))
        angles = positions.astype(F32)[:, None] * inv_freq
        sign = jnp.where(column % 2 == 0, -1.0, 1.0)
        return jnp.where(is_key, jnp.cos(angles), 1.0), jnp.where(is_key, jnp.sin(angles) * sign, 0.0)

    all_tables = (*tables(lane, True), *tables((gy % 2) * 64 + lane % 64, gy < 2))

    ring = jnp.array([0, 3, 1, 2], jnp.int32)
    place = jnp.concatenate([(x + ring) % 4, core[None]])
    source_z = (gy + ring) % 4
    at = jnp.concatenate([source_z * 2 + core, source_z * 2 + 1 - core])
    wanted = lax.dynamic_slice_in_dim(keyval_order, gy * 2, 2, 0)
    four = jnp.arange(4, dtype=jnp.int32)
    pick = jnp.concatenate(
        [jnp.array(BACK, jnp.int32)[(four - gy) % 4], jnp.stack([wanted // 2 ^ x, wanted % 2], axis=1).reshape(4), core[None]]
    )

    left, right = send(mine, along_z(1)), send(mine, along_z(-1))
    far = send(left, along_z(1))
    chunks = [spread_x(v, 1 - 2 * (p % 2)) for p, v in enumerate((mine, left, right, far))]
    q_own, q_other, kvs = [], [], []
    for n, group in enumerate(GROUPS):
        split = n + 1 == len(GROUPS)
        sums = project(place, [v for p in group for v in chunks[p]], weights, split)
        sums = [v.reshape(8, v.shape[0] // 8, v.shape[1]) for v in sums]
        if split:
            few = exchange(sums[1], "gz")
            many = exchange(sums[0], "gz")
            (kv,) = finish(finish_kv_kernel, at, (few,), all_tables[2:], (128,), n)
            own, other = finish(finish_q_kernel, at, (many, few), all_tables[:2], (width, width), n)
        else:
            came = exchange(sums[0], "gz")
            own, other, kv = finish(finish_kernel, at, (came,), all_tables, (width, width, 128), n)
        q_own.append(own)
        q_other.append(other)
        kvs.append(kv)
    q_near = jnp.concatenate(q_own[:2])
    q_near_came = send(jnp.concatenate(q_other[:2]), other_core)
    q_far_came = send(q_other[2], other_core)
    kv = spread_kv(jnp.concatenate(kvs), pick)
    kv_came = send(kv, other_core)
    return last(at, pick, (q_near, q_own[2], q_near_came, q_far_came, kv, kv_came), tokens)


def solution(mesh):
    in_specs = (
        P(("gx", "gy"), "gz"),
        P("gz"),
        P("gz", ("gx", "gy")),
        P("gz", ("gx", "gy")),
        P("gz"),
        P(),
    )
    out_specs = (P("gz", ("gx", "gy")), P("gy", "gz", None))

    return jax.shard_map(body, mesh=mesh, in_specs=in_specs, out_specs=out_specs, check_vma=False)
```
